8 devices in a mesh: dp: 1 (over z), tp: 8 (over y, x, core).
Axes of the slice: x: 2, y: 2, z: 1, core: 2. Of those that a mesh axis runs over, the one named last changes fastest.
Arguments:
- x_in: bfloat16 [32, 512, 3072], P('dp')
- adapter_ids: int32 [32], P('dp')
- gain_attn: float32 [3072], replicated
- gain_mlp: float32 [3072], replicated
- w_q: bfloat16 [3072, 24, 128], P(None, 'tp')
- w_k: bfloat16 [3072, 8, 128], P(None, 'tp')
- w_v: bfloat16 [3072, 8, 128], P(None, 'tp')
- w_o: bfloat16 [24, 128, 3072], P('tp')
- w_gate: bfloat16 [3072, 8192], P(None, 'tp')
- w_up: bfloat16 [3072, 8192], P(None, 'tp')
- w_down: bfloat16 [8192, 3072], P('tp')
- a_q: bfloat16 [16, 3072, 8], P(None, None, 'tp')
- b_q: bfloat16 [16, 8, 24, 128], P(None, None, 'tp')
- a_k: bfloat16 [16, 3072, 8], P(None, None, 'tp')
- b_k: bfloat16 [16, 8, 8, 128], P(None, None, 'tp')
- a_v: bfloat16 [16, 3072, 8], P(None, None, 'tp')
- b_v: bfloat16 [16, 8, 8, 128], P(None, None, 'tp')
- a_o: bfloat16 [16, 24, 128, 8], P(None, 'tp')
- b_o: bfloat16 [16, 8, 3072], P(None, None, 'tp')
- a_gate: bfloat16 [16, 3072, 8], P(None, None, 'tp')
- b_gate: bfloat16 [16, 8, 8192], P(None, None, 'tp')
- a_up: bfloat16 [16, 3072, 8], P(None, None, 'tp')
- b_up: bfloat16 [16, 8, 8192], P(None, None, 'tp')
- a_down: bfloat16 [16, 8192, 8], P(None, 'tp')
- b_down: bfloat16 [16, 8, 3072], P(None, None, 'tp')
Outputs:
- output: bfloat16 [32, 512, 3072], P('dp')
All inputs are finite; a program needn't handle non-finite values.
Results may differ from the reference program's by a relative error of at most 0.02.
Values are sent between devices in bfloat16 or wider.
A program may use at most 1 GiB of HBM per device.

```python
import jax
import jax.numpy as jnp
from jax import lax

BATCH = 32
SEQ_LEN = 512
D_MODEL = 3072
HEADS = 24
KV_HEADS = 8
HEAD_DIM = 128
D_FF = 8192
RANK = 8
ADAPTERS = 16
LORA_ALPHA = 16
RMS_EPS = 1e-5
Q_WIDTH = HEADS * HEAD_DIM
KV_WIDTH = KV_HEADS * HEAD_DIM


def draw_normal(rng_key, arr_shape, w_std):
    return (jax.random.normal(rng_key, arr_shape, jnp.float32) * w_std).astype(jnp.bfloat16)


def lora_pair(rng_key, a_shape, b_shape, fan_in, w_gain):
    key_a, key_b = jax.random.split(rng_key)
    a_stack = draw_normal(key_a, a_shape, fan_in ** -0.5)
    b_stack = draw_normal(key_b, b_shape, 0.2 * w_gain * RANK ** 0.5 / LORA_ALPHA)
    return a_stack, b_stack


def draw_ids(rng_key):
    key_perm, key_fill, key_mix = jax.random.split(rng_key, 3)
    id_perm = jax.random.permutation(key_perm, ADAPTERS).astype(jnp.int32)
    id_fill = jax.random.randint(key_fill, (BATCH,), 0, ADAPTERS).astype(jnp.int32)
    id_all = jnp.concatenate([id_perm, id_fill])[:BATCH]
    return jax.random.permutation(key_mix, id_all).astype(jnp.int32)


def setup_inputs(seed: int = 0, part: int = 0) -> dict:
    root_key = jax.random.key(seed)
    key_x, key_ids = jax.random.split(jax.random.fold_in(root_key, part))
    shared_keys = jax.random.split(root_key, 16)
    x_in = (0.5 * jax.random.normal(key_x, (BATCH, SEQ_LEN, D_MODEL), jnp.float32)).astype(jnp.bfloat16)
    gain_attn = 1.0 + 0.2 * jax.random.normal(shared_keys[0], (D_MODEL,), jnp.float32)
    gain_mlp = 1.0 + 0.2 * jax.random.normal(shared_keys[1], (D_MODEL,), jnp.float32)
    w_q = draw_normal(shared_keys[2], (D_MODEL, HEADS, HEAD_DIM), 1.7 * D_MODEL ** -0.5)
    w_k = draw_normal(shared_keys[3], (D_MODEL, KV_HEADS, HEAD_DIM), 1.7 * D_MODEL ** -0.5)
    w_v = draw_normal(shared_keys[4], (D_MODEL, KV_HEADS, HEAD_DIM), D_MODEL ** -0.5)
    w_o = draw_normal(shared_keys[5], (HEADS, HEAD_DIM, D_MODEL), Q_WIDTH ** -0.5)
    w_gate = draw_normal(shared_keys[6], (D_MODEL, D_FF), D_MODEL ** -0.5)
    w_up = draw_normal(shared_keys[7], (D_MODEL, D_FF), D_MODEL ** -0.5)
    w_down = draw_normal(shared_keys[8], (D_FF, D_MODEL), D_FF ** -0.5)
    a_q, b_q = lora_pair(shared_keys[9], (ADAPTERS, D_MODEL, RANK), (ADAPTERS, RANK, HEADS, HEAD_DIM), D_MODEL, 1.7)
    a_k, b_k = lora_pair(shared_keys[10], (ADAPTERS, D_MODEL, RANK), (ADAPTERS, RANK, KV_HEADS, HEAD_DIM), D_MODEL, 1.7)
    a_v, b_v = lora_pair(shared_keys[11], (ADAPTERS, D_MODEL, RANK), (ADAPTERS, RANK, KV_HEADS, HEAD_DIM), D_MODEL, 1.0)
    a_o, b_o = lora_pair(shared_keys[12], (ADAPTERS, HEADS, HEAD_DIM, RANK), (ADAPTERS, RANK, D_MODEL), Q_WIDTH, 1.0)
    a_gate, b_gate = lora_pair(shared_keys[13], (ADAPTERS, D_MODEL, RANK), (ADAPTERS, RANK, D_FF), D_MODEL, 1.0)
    a_up, b_up = lora_pair(shared_keys[14], (ADAPTERS, D_MODEL, RANK), (ADAPTERS, RANK, D_FF), D_MODEL, 1.0)
    a_down, b_down = lora_pair(shared_keys[15], (ADAPTERS, D_FF, RANK), (ADAPTERS, RANK, D_MODEL), D_FF, 1.0)
    return dict(x_in=x_in, adapter_ids=draw_ids(key_ids), gain_attn=gain_attn, gain_mlp=gain_mlp,
                w_q=w_q, w_k=w_k, w_v=w_v, w_o=w_o, w_gate=w_gate, w_up=w_up, w_down=w_down,
                a_q=a_q, b_q=b_q, a_k=a_k, b_k=b_k, a_v=a_v, b_v=b_v, a_o=a_o, b_o=b_o,
                a_gate=a_gate, b_gate=b_gate, a_up=a_up, b_up=b_up, a_down=a_down, b_down=b_down)


def rms_scale(x_in, gain_vec):
    x_f32 = x_in.astype(jnp.float32)
    inv_rms = lax.rsqrt(jnp.mean(x_f32 * x_f32, axis=-1, keepdims=True) + RMS_EPS)
    return (x_f32 * inv_rms * gain_vec).astype(jnp.bfloat16)


def lora_proj(h_in, w_base, a_sel, b_sel):
    base_out = jnp.dot(h_in, w_base, preferred_element_type=jnp.float32)
    lora_mid = jnp.dot(h_in, a_sel, preferred_element_type=jnp.float32).astype(jnp.bfloat16)
    return base_out + (LORA_ALPHA / RANK) * jnp.dot(lora_mid, b_sel, preferred_element_type=jnp.float32)


def attend_head(head_item):
    q_head, k_head, v_head = head_item
    scores = jnp.dot(q_head, k_head.T, preferred_element_type=jnp.float32) * HEAD_DIM ** -0.5
    causal = jnp.arange(SEQ_LEN)[:, None] >= jnp.arange(SEQ_LEN)[None, :]
    prob_bf = jax.nn.softmax(jnp.where(causal, scores, -jnp.inf), axis=-1).astype(jnp.bfloat16)
    return jnp.dot(prob_bf, v_head, preferred_element_type=jnp.float32).astype(jnp.bfloat16)


def reference(x_in, adapter_ids, gain_attn, gain_mlp, w_q, w_k, w_v, w_o, w_gate, w_up, w_down,
              a_q, b_q, a_k, b_k, a_v, b_v, a_o, b_o, a_gate, b_gate, a_up, b_up, a_down, b_down):
    head_group = HEADS // KV_HEADS
    w_query = w_q.reshape(D_MODEL, Q_WIDTH)
    w_key = w_k.reshape(D_MODEL, KV_WIDTH)
    w_value = w_v.reshape(D_MODEL, KV_WIDTH)
    w_out = w_o.reshape(Q_WIDTH, D_MODEL)

    def one_sequence(seq_item):
        x_seq, adapter_id = seq_item
        h_norm = rms_scale(x_seq, gain_attn)
        q_all = lora_proj(h_norm, w_query, a_q[adapter_id], b_q[adapter_id].reshape(RANK, Q_WIDTH)).astype(jnp.bfloat16)
        k_all = lora_proj(h_norm, w_key, a_k[adapter_id], b_k[adapter_id].reshape(RANK, KV_WIDTH)).astype(jnp.bfloat16)
        v_all = lora_proj(h_norm, w_value, a_v[adapter_id], b_v[adapter_id].reshape(RANK, KV_WIDTH)).astype(jnp.bfloat16)
        q_heads = q_all.reshape(SEQ_LEN, HEADS, HEAD_DIM).transpose(1, 0, 2)
        k_heads = jnp.repeat(k_all.reshape(SEQ_LEN, KV_HEADS, HEAD_DIM).transpose(1, 0, 2), head_group, axis=0)
        v_heads = jnp.repeat(v_all.reshape(SEQ_LEN, KV_HEADS, HEAD_DIM).transpose(1, 0, 2), head_group, axis=0)
        att_heads = lax.map(attend_head, (q_heads, k_heads, v_heads))
        att_flat = att_heads.transpose(1, 0, 2).reshape(SEQ_LEN, Q_WIDTH)
        z_out = lora_proj(att_flat, w_out, a_o[adapter_id].reshape(Q_WIDTH, RANK), b_o[adapter_id])
        x_one = (x_seq.astype(jnp.float32) + z_out).astype(jnp.bfloat16)
        h_two = rms_scale(x_one, gain_mlp)
        z_gate = lora_proj(h_two, w_gate, a_gate[adapter_id], b_gate[adapter_id]).astype(jnp.bfloat16)
        z_up = lora_proj(h_two, w_up, a_up[adapter_id], b_up[adapter_id]).astype(jnp.bfloat16)
        mlp_mid = (jax.nn.silu(z_gate.astype(jnp.float32)) * z_up.astype(jnp.float32)).astype(jnp.bfloat16)
        z_down = lora_proj(mlp_mid, w_down, a_down[adapter_id], b_down[adapter_id])
        return (x_one.astype(jnp.float32) + z_down).astype(jnp.bfloat16)

    return lax.map(one_sequence, (x_in, adapter_ids))
```

```python
import jax
import jax.numpy as jnp
from jax import lax
from jax.sharding import PartitionSpec as P

LORA_ALPHA = 16
RMS_EPS = 1e-5


def rms_scale(x_in, gain_vec):
    x_f32 = x_in.astype(jnp.float32)
    inv_rms = lax.rsqrt(jnp.mean(x_f32 * x_f32, axis=-1, keepdims=True) + RMS_EPS)
    return (x_f32 * inv_rms * gain_vec).astype(jnp.bfloat16)


def causal_attention(q_group, k_group, v_group):
    num_seqs, seq_len, head_dim = q_group.shape[0], q_group.shape[1], q_group.shape[-1]
    scores = jnp.einsum('bqngd,bknd->bngqk', q_group, k_group, preferred_element_type=jnp.float32) * head_dim ** -0.5
    causal = jnp.arange(seq_len)[:, None] >= jnp.arange(seq_len)[None, :]
    prob_bf = jax.nn.softmax(jnp.where(causal, scores, -jnp.inf), axis=-1).astype(jnp.bfloat16)
    att_out = jnp.einsum('bngqk,bknd->bqngd', prob_bf, v_group, preferred_element_type=jnp.float32)
    return att_out.astype(jnp.bfloat16)


def solution(mesh):
    act_spec = P('dp', None, None)
    w_head_spec = P(None, 'tp', None)
    w_out_spec = P('tp', None, None)
    w_col_spec = P(None, 'tp')
    w_row_spec = P('tp', None)
    a_rank_spec = P(None, None, 'tp')
    b_head_spec = P(None, None, 'tp', None)
    b_col_spec = P(None, None, 'tp')
    a_head_spec = P(None, 'tp', None, None)
    a_row_spec = P(None, 'tp', None)
    in_specs = (act_spec, P('dp'), P(None), P(None), w_head_spec, w_head_spec, w_head_spec, w_out_spec,
                w_col_spec, w_col_spec, w_row_spec, a_rank_spec, b_head_spec, a_rank_spec, b_head_spec,
                a_rank_spec, b_head_spec, a_head_spec, b_col_spec, a_rank_spec, b_col_spec,
                a_rank_spec, b_col_spec, a_row_spec, b_col_spec)
    n_tp = mesh.shape['tp']

    def local_layer(x_in, adapter_ids, gain_attn, gain_mlp, w_q, w_k, w_v, w_o, w_gate, w_up, w_down,
                    a_q, b_q, a_k, b_k, a_v, b_v, a_o, b_o, a_gate, b_gate, a_up, b_up, a_down, b_down):
        num_seqs, seq_len, dim = x_in.shape
        head_dim = w_q.shape[2]
        rank = b_q.shape[1]
        scale = LORA_ALPHA / rank
        n_ad = b_q.shape[0]
        per_dev = num_seqs // n_tp
        me = lax.axis_index('tp')
        x_loc = lax.dynamic_slice_in_dim(x_in, me * per_dev, per_dev, axis=0)
        ids = lax.dynamic_slice_in_dim(adapter_ids, me * per_dev, per_dev, axis=0)

        def gather(v):
            return lax.all_gather(v, 'tp', axis=0, tiled=False)

        def t_last(a):
            return jnp.swapaxes(a, -1, -2)

        qw, kw = w_q.shape[1] * head_dim, w_k.shape[1] * head_dim
        lora_attn = gather(jnp.concatenate([
            b_q.reshape(n_ad, rank, qw), b_k.reshape(n_ad, rank, kw), b_v.reshape(n_ad, rank, kw),
            t_last(a_o.reshape(n_ad, qw, rank)), b_o], axis=2))
        lora_a = gather(jnp.stack([a_q[:, :, 0], a_k[:, :, 0], a_v[:, :, 0], a_gate[:, :, 0], a_up[:, :, 0]], axis=0))
        w_qkv_all = gather(jnp.concatenate([w_q.reshape(dim, qw), w_k.reshape(dim, kw), w_v.reshape(dim, kw)], axis=1))
        w_o_all = gather(w_o.reshape(qw, dim))
        w_gate_all = gather(w_gate)
        w_up_all = gather(w_up)
        w_down_all = gather(w_down)
        lora_mlp = gather(jnp.concatenate([b_gate, b_up, t_last(a_down), b_down], axis=2))

        lora_attn = jnp.take(lora_attn, ids, axis=1)
        lora_mlp = jnp.take(lora_mlp, ids, axis=1)
        lora_a = jnp.take(lora_a, ids, axis=2)

        f32 = jnp.float32
        h = rms_scale(x_loc, gain_attn)
        t_qkv = jnp.einsum('bsd,rpbd->bspr', h, lora_a[:, :3], preferred_element_type=f32).astype(jnp.bfloat16)

        def col(h_in, w_all, t_in, b_all):
            z = jnp.einsum('bsd,gde->bsge', h_in, w_all, preferred_element_type=f32)
            return z + scale * jnp.einsum('bsr,gbre->bsge', t_in, b_all, preferred_element_type=f32)

        q = col(h, w_qkv_all[:, :, :qw], t_qkv[:, :, 0], lora_attn[..., :qw]).astype(jnp.bfloat16)
        k = col(h, w_qkv_all[:, :, qw:qw + kw], t_qkv[:, :, 1], lora_attn[..., qw:qw + kw]).astype(jnp.bfloat16)
        v = col(h, w_qkv_all[:, :, qw + kw:], t_qkv[:, :, 2], lora_attn[..., qw + kw:qw + 2 * kw]).astype(jnp.bfloat16)
        q = q.reshape(per_dev, seq_len, n_tp, qw // head_dim, head_dim)
        o = causal_attention(q, k, v).reshape(per_dev, seq_len, n_tp, qw)

        def row(u, w_all, a_t, b_all, resid):
            z = jnp.einsum('bsge,gef->bsf', u, w_all, preferred_element_type=f32)
            t = jnp.einsum('bsge,gbre->bsr', u, a_t, preferred_element_type=f32).astype(jnp.bfloat16)
            bb = jnp.moveaxis(b_all, 0, 2).reshape(per_dev, rank, dim)
            z = z + scale * jnp.einsum('bsr,brf->bsf', t, bb, preferred_element_type=f32)
            return (resid.astype(f32) + z).astype(jnp.bfloat16)

        off = qw + 2 * kw
        x_one = row(o, w_o_all, lora_attn[..., off:off + qw], lora_attn[..., off + qw:], x_loc)
        h2 = rms_scale(x_one, gain_mlp)
        t_gu = jnp.einsum('bsd,rpbd->bspr', h2, lora_a[:, 3:], preferred_element_type=f32).astype(jnp.bfloat16)
        ff = w_gate.shape[1]
        gate = col(h2, w_gate_all, t_gu[:, :, 0], lora_mlp[..., :ff]).astype(jnp.bfloat16)
        up = col(h2, w_up_all, t_gu[:, :, 1], lora_mlp[..., ff:2 * ff]).astype(jnp.bfloat16)
        mid = (jax.nn.silu(gate.astype(f32)) * up.astype(f32)).astype(jnp.bfloat16)
        y = row(mid, w_down_all, lora_mlp[..., 2 * ff:3 * ff], lora_mlp[..., 3 * ff:], x_one)
        return lax.all_gather(y, 'tp', axis=0, tiled=True)

    return jax.shard_map(local_layer, mesh=mesh, in_specs=in_specs, out_specs=act_spec, check_vma=False)
```

```python
import functools

import jax
import jax.numpy as jnp
from jax import lax
from jax.experimental import pallas as pl
from jax.experimental.pallas import tpu as pltpu
from jax.sharding import PartitionSpec as P


LORA_ALPHA = 16
RMS_EPS = 1e-5
F32 = jnp.float32
BF16 = jnp.bfloat16
CORE, XNB, YNB = 1, 2, 4
VMEM_LIMIT = 60 * 1024 * 1024

CHUNKS = [(0, 0, 256), (0, 256, 256)] + [(j, 0, 512) for j in range(1, 7)] + [(7, 0, 256), (7, 256, 256)]


def dot_nt(a, b):
    return lax.dot_general(a, b, (((1,), (1,)), ((), ())), preferred_element_type=F32)


def dot_nn(a, b):
    return lax.dot_general(a, b, (((1,), (0,)), ((), ())), preferred_element_type=F32)


def kernel_call(body, grid, in_specs, out_specs, out_shape, scratch, flops, nbytes):
    return pl.pallas_call(
        body,
        grid_spec=pltpu.PrefetchScalarGridSpec(num_scalar_prefetch=1, grid=grid, in_specs=in_specs,
                                               out_specs=out_specs, scratch_shapes=scratch),
        out_shape=out_shape,
        compiler_params=pltpu.CompilerParams(vmem_limit_bytes=VMEM_LIMIT),
        cost_estimate=pl.CostEstimate(flops=int(flops), bytes_accessed=int(nbytes), transcendentals=0))


def any_spec():
    return pl.BlockSpec(memory_space=pl.ANY)


def prep_body(meta, x_ref, g_ref, a_ref, h_ref, t_ref):
    xv = x_ref[0].astype(F32)
    inv = lax.rsqrt(jnp.mean(xv * xv, axis=-1, keepdims=True) + RMS_EPS)
    hv = (xv * inv * g_ref[...]).astype(BF16)
    h_ref[0] = hv
    t_ref[0] = dot_nt(hv, a_ref[0]).astype(BF16)


def attn_body(scale, hd, rank, meta, h_ref, t_ref, w_ref, l_ref, o_ref):
    seq = h_ref.shape[1]
    cols = w_ref.shape[1]
    kw = hd
    qw = cols - 2 * kw
    bl = l_ref[0, 0][:, :cols]
    row = lax.broadcasted_iota(jnp.int32, (3 * rank, cols), 0) // rank
    col = lax.broadcasted_iota(jnp.int32, (3 * rank, cols), 1)
    part = jnp.where(col < qw, 0, jnp.where(col < qw + kw, 1, 2))
    bd = jnp.where(row == part, jnp.concatenate([bl, bl, bl], axis=0), jnp.zeros((), BF16))
    z = dot_nn(h_ref[0], w_ref[...]) + scale * dot_nn(t_ref[0], bd)
    z = z.astype(BF16)
    kk, vv = z[:, qw:qw + kw], z[:, qw + kw:]
    half = seq // 2
    for r in range(2):
        n_key = half * (r + 1)
        ri = lax.broadcasted_iota(jnp.int32, (half, n_key), 0) + r * half
        ci = lax.broadcasted_iota(jnp.int32, (half, n_key), 1)
        keep = ri >= ci
        for j in range(qw // hd):
            s = dot_nt(z[r * half:(r + 1) * half, j * hd:(j + 1) * hd], kk[:n_key]) * hd ** -0.5
            s = jnp.where(keep, s, -jnp.inf)
            e = jnp.exp(s - jnp.max(s, axis=-1, keepdims=True))
            p = (e / jnp.sum(e, axis=-1, keepdims=True)).astype(BF16)
            o_ref[0, r * half:(r + 1) * half, j * hd:(j + 1) * hd] = dot_nn(p, vv[:n_key]).astype(BF16)


def oproj_body(n_tp, scale, qw, cols0, blk, meta, *refs):
    o_refs, w_refs = refs[:n_tp], refs[n_tp:2 * n_tp]
    x_ref, l_ref, x1_ref, ocat, acat, bcat, wbuf, sems = refs[2 * n_tp:]
    dim = ocat.shape[1]
    n_blk = dim // blk
    me = meta[0]

    def copies(n, slot):
        return [pltpu.make_async_copy(w_refs[p].at[:, pl.ds(n * blk, blk)], wbuf.at[slot, pl.ds(p * qw, qw)],
                                      sems.at[slot]) for p in range(n_tp)]

    for c in copies(0, 0):
        c.start()
    for p in range(n_tp):
        ocat[:, p * qw:(p + 1) * qw] = o_refs[p][0]
        acat[:, p * qw:(p + 1) * qw] = l_ref[p, 0, :, cols0:cols0 + qw]
        bcat[:, p * qw:(p + 1) * qw] = l_ref[jnp.bitwise_xor(me, p), 0, :, cols0 + qw:cols0 + 2 * qw]
    t = dot_nt(ocat[...], acat[...]).astype(BF16)

    @pl.loop(0, n_blk)
    def _(n):
        slot = lax.rem(n, 2)

        @pl.when(n + 1 < n_blk)
        def _():
            for c in copies(n + 1, 1 - slot):
                c.start()

        for c in copies(n, slot):
            c.wait()
        cols = pl.ds(pl.multiple_of(n * blk, blk), blk)
        z = dot_nn(ocat[...], wbuf[slot]) + scale * dot_nn(t, bcat[:, cols])
        x1_ref[:, cols] = (x_ref[0, :, cols].astype(F32) + z).astype(BF16)


def pick(meta, which, own_ref, nbr_ref, dst, sem):
    own = meta[1] == which

    @pl.when(own)
    def _():
        pltpu.make_async_copy(own_ref, dst, sem).start()

    @pl.when(jnp.logical_not(own))
    def _():
        pltpu.make_async_copy(nbr_ref, dst, sem).start()

    return pltpu.make_async_copy(own_ref, dst, sem)


def gu_body(n_p, scale, rank, blk, which, meta, xo_ref, xn_ref, g_ref, a_ref, *refs):
    b_refs, g_refs, u_refs = refs[:n_p], refs[n_p:2 * n_p], refs[2 * n_p:3 * n_p]
    m_ref, hbuf, bcat, wbuf, sems, sem_x = refs[3 * n_p:]
    ff = g_refs[0].shape[1]
    per = ff // blk
    n_blk = n_p * per

    def start(j, slot):
        for p in range(n_p):
            @pl.when(j // per == p)
            def _():
                cols = pl.ds(pl.multiple_of(lax.rem(j, per) * blk, blk), blk)
                pltpu.make_async_copy(g_refs[p].at[:, cols], wbuf.at[slot, 0], sems.at[slot, 0]).start()
                pltpu.make_async_copy(u_refs[p].at[:, cols], wbuf.at[slot, 1], sems.at[slot, 1]).start()

    fetch = pick(meta, which, xo_ref, xn_ref, hbuf, sem_x)
    start(0, 0)
    zero = jnp.zeros((rank, ff), BF16)
    for p in range(n_p):
        bcat[0, :, p * ff:(p + 1) * ff] = jnp.concatenate([b_refs[p][0, :, :ff], zero], axis=0)
        bcat[1, :, p * ff:(p + 1) * ff] = jnp.concatenate([zero, b_refs[p][0, :, ff:2 * ff]], axis=0)
    fetch.wait()
    xv = hbuf[...].astype(F32)
    inv = lax.rsqrt(jnp.mean(xv * xv, axis=-1, keepdims=True) + RMS_EPS)
    hbuf[...] = (xv * inv * g_ref[...]).astype(BF16)
    t = dot_nt(hbuf[...], a_ref[0]).astype(BF16)

    @pl.loop(0, n_blk)
    def _(j):
        slot = lax.rem(j, 2)

        @pl.when(j + 1 < n_blk)
        def _():
            start(j + 1, 1 - slot)

        cols = pl.ds(pl.multiple_of(j * blk, blk), blk)
        z = []
        for i in range(2):
            pltpu.make_async_copy(g_refs[0].at[:, pl.ds(0, blk)], wbuf.at[slot, i], sems.at[slot, i]).wait()
            z.append((dot_nn(hbuf[...], wbuf[slot, i]) + scale * dot_nn(t, bcat[i, :, cols])).astype(BF16))
        gate, up = z[0].astype(F32), z[1].astype(F32)
        m_ref[:, cols] = (jax.nn.silu(gate) * up).astype(BF16)


def down_body(n_p, blk, b_off, meta, m_ref, *refs):
    b_refs, d_refs = refs[:n_p], refs[n_p:2 * n_p]
    p_ref, t_ref, acat, wbuf, sems = refs[2 * n_p:]
    ff, dim = d_refs[0].shape
    n_blk = dim // blk

    def copies(n, slot):
        return [pltpu.make_async_copy(d_refs[p].at[:, pl.ds(n * blk, blk)], wbuf.at[slot, pl.ds(p * ff, ff)],
                                      sems.at[slot]) for p in range(n_p)]

    for c in copies(0, 0):
        c.start()
    for p in range(n_p):
        acat[:, p * ff:(p + 1) * ff] = b_refs[p][0, :, b_off:b_off + ff]
    t_ref[...] = dot_nt(m_ref[...], acat[...]).T

    @pl.loop(0, n_blk)
    def _(n):
        slot = lax.rem(n, 2)

        @pl.when(n + 1 < n_blk)
        def _():
            for c in copies(n + 1, 1 - slot):
                c.start()

        for c in copies(n, slot):
            c.wait()
        p_ref[:, pl.ds(pl.multiple_of(n * blk, blk), blk)] = dot_nn(m_ref[...], wbuf[slot]).astype(BF16)


def fin_body(scale, l_off, qw, which, row0, meta, pa_ref, pb_ref, ta_ref, tb_ref, l_ref, xo_ref, xn_ref,
             y_ref, xbuf, bcat, sem_x):
    rows = pl.ds(row0, y_ref.shape[0])
    fetch = pick(meta, which, xo_ref.at[rows], xn_ref.at[rows], xbuf, sem_x)
    me = meta[0]
    for p in range(l_ref.shape[0]):
        bcat[:, p * qw:(p + 1) * qw] = l_ref[jnp.bitwise_xor(me, p), 0, :, l_off:l_off + qw]
    t = (ta_ref[...] + tb_ref[...]).T.astype(BF16)
    z = pa_ref[...].astype(F32) + pb_ref[...].astype(F32) + scale * dot_nn(t, bcat[...])
    fetch.wait()
    y_ref[...] = (xbuf[...].astype(F32) + z).astype(BF16)


def solution(mesh):
    act_spec = P('dp', None, None)
    w_head_spec = P(None, 'tp', None)
    w_out_spec = P('tp', None, None)
    w_col_spec = P(None, 'tp')
    w_row_spec = P('tp', None)
    a_rank_spec = P(None, None, 'tp')
    b_head_spec = P(None, None, 'tp', None)
    b_col_spec = P(None, None, 'tp')
    a_head_spec = P(None, 'tp', None, None)
    a_row_spec = P(None, 'tp', None)
    in_specs = (act_spec, P('dp'), P(None), P(None), w_head_spec, w_head_spec, w_head_spec, w_out_spec,
                w_col_spec, w_col_spec, w_row_spec, a_rank_spec, b_head_spec, a_rank_spec, b_head_spec,
                a_rank_spec, b_head_spec, a_head_spec, b_col_spec, a_rank_spec, b_col_spec,
                a_rank_spec, b_col_spec, a_row_spec, b_col_spec)
    n_tp = mesh.shape['tp']

    def local_layer(x_in, adapter_ids, gain_attn, gain_mlp, w_q, w_k, w_v, w_o, w_gate, w_up, w_down,
                    a_q, b_q, a_k, b_k, a_v, b_v, a_o, b_o, a_gate, b_gate, a_up, b_up, a_down, b_down):
        num_seqs, seq, dim = x_in.shape
        hd = w_q.shape[2]
        n_ad, rank = b_q.shape[:2]
        scale = LORA_ALPHA / rank
        per = num_seqs // n_tp
        ff = w_gate.shape[1]
        qw, kw = w_q.shape[1] * hd, w_k.shape[1] * hd
        cols = qw + 2 * kw
        me = lax.axis_index('tp')

        def hop(v, mask):
            return lax.ppermute(v, 'tp', [(i, i ^ mask) for i in range(n_tp)])

        def t_last(a):
            return jnp.swapaxes(a, -1, -2)

        ids_own = lax.dynamic_slice_in_dim(adapter_ids, me * per, per)
        xbit = (me // XNB) % 2
        ids_w = [lax.dynamic_slice_in_dim(adapter_ids, (me + (w - xbit) * XNB) * per, per) for w in range(2)]
        meta = jnp.concatenate([jnp.stack([me, xbit]).astype(jnp.int32), ids_own, jnp.stack(ids_w, axis=1).reshape(-1)])
        own0, slot0 = 2, 2 + per

        lora_pack = jnp.concatenate([
            b_q.reshape(n_ad, rank, qw), b_k.reshape(n_ad, rank, kw), b_v.reshape(n_ad, rank, kw),
            t_last(a_o.reshape(n_ad, qw, rank)), b_o, b_down], axis=2)
        a_pack = jnp.stack([a_q[:, :, 0], a_k[:, :, 0], a_v[:, :, 0], a_gate[:, :, 0], a_up[:, :, 0]], axis=0)
        la, lb = {0: a_pack}, {0: lora_pack}
        for src, mask, dst in ((0, YNB, YNB), (0, XNB, XNB), (0, CORE, CORE), (XNB, CORE, 3),
                                     (YNB, CORE, 5)):
            la[dst] = hop(la[src], mask)
            lb[dst] = hop(lb[src], mask)
        la[6] = hop(la[YNB], XNB)
        lb[6] = hop(lb[XNB], YNB)
        la[7] = hop(la[6], CORE)
        lb[7] = hop(lb[6], CORE)
        lora = jnp.stack([lb[d] for d in range(n_tp)])
        a_all = jnp.take(jnp.stack([la[d] for d in range(n_tp)]), jnp.bitwise_xor(me, jnp.arange(n_tp)), axis=0)
        a_qkv = jnp.transpose(a_all[:, :3], (2, 1, 0, 3)).reshape(n_ad, 3 * rank, dim)
        a_gu = jnp.transpose(a_all[:, 3:], (2, 1, 0, 3)).reshape(n_ad, 2 * rank, dim)
        mlp_pack = jnp.concatenate([b_gate, b_up, t_last(a_down)], axis=2)

        w_qkv = jnp.concatenate([w_q.reshape(dim, qw), w_k.reshape(dim, kw), w_v.reshape(dim, kw)], axis=1)
        att = {0: (w_qkv, w_o.reshape(qw, dim))}

        def move(pieces, src, mask):
            pieces[src ^ mask] = tuple(hop(v, mask) for v in pieces[src])

        move(att, 0, YNB)
        move(att, 0, XNB)
        move(att, 0, CORE)
        move(att, YNB, XNB)
        move(att, XNB, CORE)
        move(att, YNB, CORE)
        move(att, YNB ^ XNB, CORE)
        mlp = {0: (w_gate, w_up, w_down, mlp_pack)}
        move(mlp, 0, YNB)
        move(mlp, 0, CORE)
        move(mlp, YNB, CORE)
        mlp_order = (0, CORE, YNB, YNB ^ CORE)

        h, t_qkv = kernel_call(
            prep_body, (per,),
            [pl.BlockSpec((1, seq, dim), lambda i, m: (m[0] * per + i, 0, 0)),
             pl.BlockSpec((1, dim), lambda i, m: (0, 0)),
             pl.BlockSpec((1, 3 * rank, dim), lambda i, m: (m[own0 + i], 0, 0))],
            [pl.BlockSpec((1, seq, dim), lambda i, m: (i, 0, 0)),
             pl.BlockSpec((1, seq, 3 * rank), lambda i, m: (i, 0, 0))],
            [jax.ShapeDtypeStruct((per, seq, dim), BF16), jax.ShapeDtypeStruct((per, seq, 3 * rank), BF16)],
            [], 2 * per * seq * dim * 256, 4 * per * seq * dim,
        )(meta, x_in, gain_attn[None], a_qkv)

        def attn(d, first, n):
            return kernel_call(
                functools.partial(attn_body, scale, hd, rank), (n,),
                [pl.BlockSpec((1, seq, dim), lambda i, m: (first + i, 0, 0)),
                 pl.BlockSpec((1, seq, 3 * rank), lambda i, m: (first + i, 0, 0)),
                 pl.BlockSpec((dim, cols), lambda i, m: (0, 0)),
                 pl.BlockSpec((1, 1, rank, lora.shape[3]), lambda i, m: (d, m[own0 + first + i], 0, 0))],
                pl.BlockSpec((1, seq, qw), lambda i, m: (i, 0, 0)),
                jax.ShapeDtypeStruct((n, seq, qw), BF16),
                [], 2 * n * seq * dim * cols * 2, 2 * (n * seq * (dim + qw) + dim * cols),
            )(meta, h, t_qkv, att[d][0], lora)

        whole = [attn(d, 0, per) for d in range(6)]
        x1, x1n = [], []
        blk = 512
        for i in range(per):
            parts = whole + [attn(d, i, 1) for d in (6, 7)]
            x1.append(kernel_call(
                functools.partial(oproj_body, n_tp, scale, qw, cols, blk), (1,),
                [pl.BlockSpec((1, seq, qw), lambda g, m, i=i if d < 6 else 0: (i, 0, 0)) for d in range(n_tp)]
                + [any_spec()] * n_tp
                + [pl.BlockSpec((1, seq, dim), lambda g, m, i=i: (m[0] * per + i, 0, 0)),
                   pl.BlockSpec((n_tp, 1, rank, lora.shape[3]), lambda g, m, i=i: (0, m[own0 + i], 0, 0))],
                pl.BlockSpec((seq, dim), lambda g, m: (0, 0)),
                jax.ShapeDtypeStruct((seq, dim), BF16),
                [pltpu.VMEM((seq, dim), BF16), pltpu.VMEM((rank, dim), BF16), pltpu.VMEM((rank, dim), BF16),
                 pltpu.VMEM((2, dim, blk), BF16), pltpu.SemaphoreType.DMA((2,))],
                2 * seq * dim * dim, 2 * (4 * seq * dim + dim * dim),
            )(meta, *parts, *[att[d][1] for d in range(n_tp)], x_in, lora))
            x1n.append(hop(x1[i], XNB))

        n_p = len(mlp_order)
        full = lambda g, m: (0, 0)

        def gate_up(j):
            return kernel_call(
                functools.partial(gu_body, n_p, scale, rank, blk, j % 2), (1,),
                [any_spec(), any_spec(), pl.BlockSpec((1, dim), full),
                 pl.BlockSpec((1, 2 * rank, dim), lambda g, m: (m[slot0 + j], 0, 0))]
                + [pl.BlockSpec((1, rank, 3 * ff), lambda g, m: (m[slot0 + j], 0, 0))] * n_p
                + [any_spec()] * (2 * n_p),
                pl.BlockSpec((seq, n_p * ff), full),
                jax.ShapeDtypeStruct((seq, n_p * ff), BF16),
                [pltpu.VMEM((seq, dim), BF16), pltpu.VMEM((2, 2 * rank, n_p * ff), BF16),
                 pltpu.VMEM((2, 2, dim, blk), BF16), pltpu.SemaphoreType.DMA((2, 2)), pltpu.SemaphoreType.DMA],
                4 * seq * dim * n_p * ff, 2 * (seq * (dim + n_p * ff) + 2 * dim * n_p * ff),
            )(meta, x1[j // 2], x1n[j // 2], gain_mlp[None], a_gu, *[mlp[d][3] for d in mlp_order],
              *[mlp[d][0] for d in mlp_order], *[mlp[d][1] for d in mlp_order])

        def down(mid, c):
            j, row0, rows = CHUNKS[c]
            return kernel_call(
                functools.partial(down_body, n_p, blk, 2 * ff), (1,),
                [pl.BlockSpec((rows, n_p * ff), lambda g, m: (row0 // rows, 0))]
                + [pl.BlockSpec((1, rank, 3 * ff), lambda g, m: (m[slot0 + j], 0, 0))] * n_p + [any_spec()] * n_p,
                [pl.BlockSpec((rows, dim), full), pl.BlockSpec((rank, rows), full)],
                [jax.ShapeDtypeStruct((rows, dim), BF16), jax.ShapeDtypeStruct((rank, rows), F32)],
                [pltpu.VMEM((rank, n_p * ff), BF16), pltpu.VMEM((2, n_p * ff, blk), BF16),
                 pltpu.SemaphoreType.DMA((2,))],
                2 * rows * dim * n_p * ff, 2 * (rows * (dim + n_p * ff) + dim * n_p * ff),
            )(meta, mid, *[mlp[d][3] for d in mlp_order], *[mlp[d][2] for d in mlp_order])

        def final(c, pa, pb, ta, tb):
            j, row0, rows = CHUNKS[c]
            return kernel_call(
                functools.partial(fin_body, scale, cols + 2 * qw, qw, j % 2, row0), (1,),
                [pl.BlockSpec((rows, dim), full)] * 2 + [pl.BlockSpec((rank, rows), full)] * 2
                + [pl.BlockSpec((n_tp, 1, rank, lora.shape[3]), lambda g, m: (0, m[slot0 + j], 0, 0)),
                   any_spec(), any_spec()],
                pl.BlockSpec((rows, dim), full), jax.ShapeDtypeStruct((rows, dim), BF16),
                [pltpu.VMEM((rows, dim), BF16), pltpu.VMEM((rank, dim), BF16), pltpu.SemaphoreType.DMA],
                2 * rows * dim * 256, 8 * rows * dim,
            )(meta, pa, pb, ta, tb, lora, x1[j // 2], x1n[j // 2])

        def place(buf, c, pieces):
            j, row0, rows = CHUNKS[c]
            masks = list(pieces)
            n = len(masks)

            def body(meta, *refs):
                src, dst, vbuf, sem_in, sem_out = refs[:n], refs[n + 1], refs[n + 2], refs[n + 3], refs[n + 4]
                base = meta[0] + (j % 2 - meta[1]) * XNB
                ins = [pltpu.make_async_copy(src[k], vbuf.at[k], sem_in.at[k]) for k in range(n)]
                outs = [pltpu.make_async_copy(
                    vbuf.at[k], dst.at[jnp.bitwise_xor(base, masks[k]) * per + j // 2, pl.ds(row0, rows)],
                    sem_out.at[k]) for k in range(n)]
                for cp in ins:
                    cp.start()
                for k in range(n):
                    ins[k].wait()
                    outs[k].start()
                for cp in outs:
                    cp.wait()

            return pl.pallas_call(
                body,
                grid_spec=pltpu.PrefetchScalarGridSpec(
                    num_scalar_prefetch=1, grid=(1,), in_specs=[any_spec()] * (n + 1), out_specs=any_spec(),
                    scratch_shapes=[pltpu.VMEM((n, rows, dim), BF16), pltpu.SemaphoreType.DMA((n,)),
                                    pltpu.SemaphoreType.DMA((n,))]),
                out_shape=jax.ShapeDtypeStruct(buf.shape, BF16),
                input_output_aliases={n + 1: 0},
                compiler_params=pltpu.CompilerParams(vmem_limit_bytes=VMEM_LIMIT),
                cost_estimate=pl.CostEstimate(flops=10 ** 9, bytes_accessed=4 * n * rows * dim, transcendentals=0))(meta, *[pieces[d] for d in masks], buf)

        out = pl.pallas_call(lambda o_ref: None, out_shape=jax.ShapeDtypeStruct(x_in.shape, BF16),
                             out_specs=any_spec(), name="buffer")()
        mids = [gate_up(j) for j in range(2 * per)]
        for c in range(len(CHUNKS)):
            pa, ta = down(mids[CHUNKS[c][0]], c)
            y = final(c, pa, hop(pa, XNB), ta, hop(ta, XNB))
            yy = hop(y, YNB)
            out = place(out, c, {0: y, CORE: hop(y, CORE), YNB: yy, YNB ^ CORE: hop(yy, CORE)})
        return out

    return jax.shard_map(local_layer, mesh=mesh, in_specs=in_specs, out_specs=act_spec, check_vma=False)
```

```python
import functools

import jax
import jax.numpy as jnp
from jax import lax
from jax.experimental import pallas as pl
from jax.experimental.pallas import tpu as pltpu
from jax.sharding import PartitionSpec as P


LORA_ALPHA = 16
RMS_EPS = 1e-5
F32 = jnp.float32
BF16 = jnp.bfloat16
CORE, XNB, YNB = 1, 2, 4
VMEM_LIMIT = 60 * 1024 * 1024

CHUNKS = ([(0, 0, 128), (0, 128, 128), (0, 256, 256)] + [(j, 0, 512) for j in range(1, 7)]
          + [(7, 0, 256), (7, 256, 128), (7, 384, 128)])
DOWNS = [(0, 1), (2,), (3,), (4,), (5,), (6,), (7,), (8,), (9, 10, 11)]


def dot_nt(a, b):
    return lax.dot_general(a, b, (((1,), (1,)), ((), ())), preferred_element_type=F32)


def dot_nn(a, b):
    return lax.dot_general(a, b, (((1,), (0,)), ((), ())), preferred_element_type=F32)


def kernel_call(body, grid, in_specs, out_specs, out_shape, scratch, flops, nbytes):
    return pl.pallas_call(
        body,
        grid_spec=pltpu.PrefetchScalarGridSpec(num_scalar_prefetch=1, grid=grid, in_specs=in_specs,
                                               out_specs=out_specs, scratch_shapes=scratch),
        out_shape=out_shape,
        compiler_params=pltpu.CompilerParams(vmem_limit_bytes=VMEM_LIMIT),
        cost_estimate=pl.CostEstimate(flops=int(flops), bytes_accessed=int(nbytes), transcendentals=0))


def any_spec():
    return pl.BlockSpec(memory_space=pl.ANY)


def prep_body(meta, x_ref, g_ref, a_ref, h_ref, t_ref):
    xv = x_ref[0].astype(F32)
    inv = lax.rsqrt(jnp.mean(xv * xv, axis=-1, keepdims=True) + RMS_EPS)
    hv = (xv * inv * g_ref[...]).astype(BF16)
    h_ref[0] = hv
    t_ref[0] = dot_nt(hv, a_ref[0]).astype(BF16)


def rank_dot(a, b):
    n = a.shape[0] // 2
    return jnp.concatenate([dot_nt(a[:n], b), dot_nt(a[n:], b)], axis=0)


def softmax_bf16(blocks, scale):
    m = functools.reduce(jnp.maximum, [jnp.max(s, axis=-1, keepdims=True) for s in blocks])
    e = [jnp.exp2((s - m) * (scale * 1.4426950408889634)) for s in blocks]
    inv = 1.0 / functools.reduce(jnp.add, [jnp.sum(v, axis=-1, keepdims=True) for v in e])
    return [(v * inv).astype(BF16) for v in e]


def attn_body(scale, hd, rank, n_w, meta, h_ref, t_ref, *refs):
    w_refs, l_refs, o_refs = refs[:n_w], refs[n_w:2 * n_w], refs[2 * n_w:]
    seq = h_ref.shape[1]
    cols = w_refs[0].shape[1]
    qw = cols - 2 * hd
    half = seq // 2
    row = lax.broadcasted_iota(jnp.int32, (3 * rank, cols), 0) // rank
    col = lax.broadcasted_iota(jnp.int32, (3 * rank, cols), 1)
    part = jnp.where(col < qw, 0, jnp.where(col < qw + hd, 1, 2))
    keep = (lax.broadcasted_iota(jnp.int32, (half, half), 0) >= lax.broadcasted_iota(jnp.int32, (half, half), 1))
    zs = []
    for w_ref, l_ref in zip(w_refs, l_refs):
        bl = l_ref[0, 0][:, :cols]
        bd = jnp.where(row == part, jnp.concatenate([bl, bl, bl], axis=0), jnp.zeros((), BF16))
        zs.append((dot_nn(h_ref[0], w_ref[...]) + scale * dot_nn(t_ref[0], bd)).astype(BF16))
    for z, o_ref in zip(zs, o_refs):
        k = [z[r * half:(r + 1) * half, qw:qw + hd] for r in range(2)]
        v = [z[r * half:(r + 1) * half, qw + hd:] for r in range(2)]
        for j in range(qw // hd):
            for r in range(2):
                q = z[r * half:(r + 1) * half, j * hd:(j + 1) * hd]
                s = [dot_nt(q, k[c]) for c in range(r + 1)]
                s[r] = jnp.where(keep, s[r], -jnp.inf)
                p = softmax_bf16(s, hd ** -0.5)
                o = functools.reduce(jnp.add, [dot_nn(p[c], v[c]) for c in range(r + 1)])
                o_ref[0, r * half:(r + 1) * half, j * hd:(j + 1) * hd] = o.astype(BF16)


def twice(scale, t):
    return [t] * int(scale)


def oproj_body(n_tp, scale, qw, cols0, blk, ext, meta, *refs):
    o_refs, w_refs = refs[:n_tp], refs[n_tp:2 * n_tp]
    x_ref, l_ref, x1_ref, ocat, acat, bcat, wbuf, sems = refs[2 * n_tp:]
    dim = x1_ref.shape[1]
    rank = acat.shape[0]
    n_blk = dim // blk
    me = meta[0]

    def copies(n, slot):
        return [pltpu.make_async_copy(w_refs[p].at[:, pl.ds(n * blk, blk)], wbuf.at[slot, pl.ds(p * qw, qw)],
                                      sems.at[slot]) for p in range(n_tp)]

    for c in copies(0, 0):
        c.start()
    bcat[...] = jnp.zeros_like(bcat)
    for p in range(n_tp):
        ocat[:, p * qw:(p + 1) * qw] = o_refs[p][0]
        acat[:, p * qw:(p + 1) * qw] = l_ref[p, 0, :, cols0:cols0 + qw]
        b = l_ref[jnp.bitwise_xor(me, p), 0, :, cols0 + qw:cols0 + 2 * qw]
        bcat[:2 * rank, p * qw:(p + 1) * qw] = jnp.concatenate(twice(scale, b), axis=0)
    t = rank_dot(ocat[:, :dim], acat[...]).astype(BF16)
    pad = jnp.zeros((t.shape[0], ext - 2 * rank), BF16)
    ocat[:, dim:] = jnp.concatenate(twice(scale, t) + [pad], axis=1)

    @pl.loop(0, n_blk)
    def _(n):
        slot = lax.rem(n, 2)

        @pl.when(n + 1 < n_blk)
        def _():
            for c in copies(n + 1, 1 - slot):
                c.start()

        cols = pl.ds(pl.multiple_of(n * blk, blk), blk)
        wbuf[slot, dim:] = bcat[:, cols]
        for c in copies(n, slot):
            c.wait()
        z = dot_nn(ocat[...], wbuf[slot])
        x1_ref[:, cols] = (x_ref[0, :, cols].astype(F32) + z).astype(BF16)


def pick(meta, which, own_ref, nbr_ref, dst, sem):
    own = meta[1] == which

    @pl.when(own)
    def _():
        pltpu.make_async_copy(own_ref, dst, sem).start()

    @pl.when(jnp.logical_not(own))
    def _():
        pltpu.make_async_copy(nbr_ref, dst, sem).start()

    return pltpu.make_async_copy(own_ref, dst, sem)


def gu_body(n_p, scale, rank, blk, ext, which, meta, xo_ref, xn_ref, g_ref, a_ref, *refs):
    b_refs, g_refs, u_refs = refs[:n_p], refs[n_p:2 * n_p], refs[2 * n_p:3 * n_p]
    m_ref, hbuf, bcat, wbuf, zbuf, sems, sem_x = refs[3 * n_p:]
    ff = g_refs[0].shape[1]
    dim = xo_ref.shape[1]
    per = ff // blk
    n_blk = n_p * per

    def start(j, slot):
        for p in range(n_p):
            @pl.when(j // per == p)
            def _():
                cols = pl.ds(pl.multiple_of(lax.rem(j, per) * blk, blk), blk)
                for i, w in enumerate((g_refs[p], u_refs[p])):
                    pltpu.make_async_copy(w.at[:, cols], wbuf.at[slot, i, pl.ds(0, dim)], sems.at[slot, i]).start()

    fetch = pick(meta, which, xo_ref, xn_ref, hbuf.at[:, pl.ds(0, dim)], sem_x)
    start(0, 0)
    zero = jnp.zeros((2 * rank, ff), BF16)
    rest = jnp.zeros((ext - 4 * rank, ff), BF16)
    for p in range(n_p):
        bg = twice(scale, b_refs[p][0, :, :ff])
        bu = twice(scale, b_refs[p][0, :, ff:2 * ff])
        bcat[0, :, p * ff:(p + 1) * ff] = jnp.concatenate(bg + [zero, rest], axis=0)
        bcat[1, :, p * ff:(p + 1) * ff] = jnp.concatenate([zero] + bu + [rest], axis=0)
    fetch.wait()
    xv = hbuf[:, :dim].astype(F32)
    inv = lax.rsqrt(jnp.mean(xv * xv, axis=-1, keepdims=True) + RMS_EPS)
    hbuf[:, :dim] = (xv * inv * g_ref[...]).astype(BF16)
    t = rank_dot(hbuf[:, :dim], a_ref[0]).astype(BF16)
    pad = jnp.zeros((t.shape[0], ext - 4 * rank), BF16)
    hbuf[:, dim:] = jnp.concatenate(twice(scale, t[:, :rank]) + twice(scale, t[:, rank:]) + [pad], axis=1)

    def act(j):
        gate, up = zbuf[0].astype(F32), zbuf[1].astype(F32)
        m_ref[:, pl.ds(pl.multiple_of(j * blk, blk), blk)] = (jax.nn.silu(gate) * up).astype(BF16)

    zbuf[...] = jnp.zeros_like(zbuf)

    @pl.loop(0, n_blk)
    def _(j):
        slot = lax.rem(j, 2)

        @pl.when(j + 1 < n_blk)
        def _():
            start(j + 1, 1 - slot)

        cols = pl.ds(pl.multiple_of(j * blk, blk), blk)
        for i in range(2):
            wbuf[slot, i, dim:] = bcat[i, :, cols]
            pltpu.make_async_copy(g_refs[0].at[:, pl.ds(0, blk)], wbuf.at[slot, i, pl.ds(0, dim)],
                                  sems.at[slot, i]).wait()
        act(jnp.maximum(j - 1, 0))
        for i in range(2):
            zbuf[i] = dot_nn(hbuf[...], wbuf[slot, i]).astype(BF16)

    act(n_blk - 1)


def down_body(n_p, blk, b_off, splits, meta, m_ref, *refs):
    b_refs, d_refs = refs[:n_p], refs[n_p:2 * n_p]
    refs = refs[2 * n_p:]
    k = len(splits)
    p_refs, t_refs, (acat, wbuf, sems) = refs[:k], refs[k:2 * k], refs[2 * k:]
    ff, dim = d_refs[0].shape
    n_blk = dim // blk

    def copies(n, slot):
        return [pltpu.make_async_copy(d_refs[p].at[:, pl.ds(n * blk, blk)], wbuf.at[slot, pl.ds(p * ff, ff)],
                                      sems.at[slot]) for p in range(n_p)]

    for c in copies(0, 0):
        c.start()
    for p in range(n_p):
        acat[:, p * ff:(p + 1) * ff] = b_refs[p][0, :, b_off:b_off + ff]
    t = rank_dot(m_ref[...], acat[...]).T
    row = 0
    for n, t_ref in zip(splits, t_refs):
        t_ref[...] = t[:, row:row + n]
        row += n

    @pl.loop(0, n_blk)
    def _(n):
        slot = lax.rem(n, 2)

        @pl.when(n + 1 < n_blk)
        def _():
            for c in copies(n + 1, 1 - slot):
                c.start()

        for c in copies(n, slot):
            c.wait()
        z = dot_nn(m_ref[...], wbuf[slot]).astype(BF16)
        row = 0
        for rows, p_ref in zip(splits, p_refs):
            p_ref[:, pl.ds(pl.multiple_of(n * blk, blk), blk)] = z[row:row + rows]
            row += rows


def fin_body(scale, l_off, qw, which, row0, meta, pa_ref, pb_ref, ta_ref, tb_ref, l_ref, xo_ref, xn_ref,
             y_ref, xbuf, bcat, sem_x):
    i = pl.program_id(0)
    sub = y_ref.shape[0]
    n = xbuf.shape[0] // sub

    def fetch(b):
        rows = pl.ds(row0 + b * sub, sub)
        return pick(meta, which, xo_ref.at[rows], xn_ref.at[rows], xbuf.at[pl.ds(b * sub, sub)], sem_x.at[b])

    @pl.when(i == 0)
    def _():
        for b in range(n):
            fetch(b)
        for p in range(l_ref.shape[0]):
            bcat[:, p * qw:(p + 1) * qw] = l_ref[jnp.bitwise_xor(meta[0], p), 0, :, l_off:l_off + qw]

    t = (ta_ref[...] + tb_ref[...]).T.astype(BF16)
    z = pa_ref[...].astype(F32) + pb_ref[...].astype(F32) + scale * dot_nn(t, bcat[...])
    mine = pl.ds(pl.multiple_of(i * sub, sub), sub)
    pltpu.make_async_copy(xo_ref.at[pl.ds(0, sub)], xbuf.at[mine], sem_x.at[i]).wait()
    y_ref[...] = (xbuf[mine].astype(F32) + z).astype(BF16)


def solution(mesh):
    act_spec = P('dp', None, None)
    w_head_spec = P(None, 'tp', None)
    w_out_spec = P('tp', None, None)
    w_col_spec = P(None, 'tp')
    w_row_spec = P('tp', None)
    a_rank_spec = P(None, None, 'tp')
    b_head_spec = P(None, None, 'tp', None)
    b_col_spec = P(None, None, 'tp')
    a_head_spec = P(None, 'tp', None, None)
    a_row_spec = P(None, 'tp', None)
    in_specs = (act_spec, P('dp'), P(None), P(None), w_head_spec, w_head_spec, w_head_spec, w_out_spec,
                w_col_spec, w_col_spec, w_row_spec, a_rank_spec, b_head_spec, a_rank_spec, b_head_spec,
                a_rank_spec, b_head_spec, a_head_spec, b_col_spec, a_rank_spec, b_col_spec,
                a_rank_spec, b_col_spec, a_row_spec, b_col_spec)
    n_tp = mesh.shape['tp']

    def local_layer(x_in, adapter_ids, gain_attn, gain_mlp, w_q, w_k, w_v, w_o, w_gate, w_up, w_down,
                    a_q, b_q, a_k, b_k, a_v, b_v, a_o, b_o, a_gate, b_gate, a_up, b_up, a_down, b_down):
        num_seqs, seq, dim = x_in.shape
        hd = w_q.shape[2]
        n_ad, rank = b_q.shape[:2]
        scale = LORA_ALPHA / rank
        per = num_seqs // n_tp
        ff = w_gate.shape[1]
        qw, kw = w_q.shape[1] * hd, w_k.shape[1] * hd
        cols = qw + 2 * kw
        me = lax.axis_index('tp')

        def hop(v, mask):
            return lax.ppermute(v, 'tp', [(i, i ^ mask) for i in range(n_tp)])

        def t_last(a):
            return jnp.swapaxes(a, -1, -2)

        ids_own = lax.dynamic_slice_in_dim(adapter_ids, me * per, per)
        xbit = (me // XNB) % 2
        ids_w = [lax.dynamic_slice_in_dim(adapter_ids, (me + (w - xbit) * XNB) * per, per) for w in range(2)]
        meta = jnp.concatenate([jnp.stack([me, xbit]).astype(jnp.int32), ids_own, jnp.stack(ids_w, axis=1).reshape(-1)])
        own0, slot0 = 2, 2 + per

        lora_pack = jnp.concatenate([
            b_q.reshape(n_ad, rank, qw), b_k.reshape(n_ad, rank, kw), b_v.reshape(n_ad, rank, kw),
            t_last(a_o.reshape(n_ad, qw, rank)), b_o, b_down], axis=2)
        a_pack = jnp.stack([a_q[:, :, 0], a_k[:, :, 0], a_v[:, :, 0], a_gate[:, :, 0], a_up[:, :, 0]], axis=0)
        la, lb = {0: a_pack}, {0: lora_pack}
        for src, mask, dst in ((0, YNB, YNB), (0, XNB, XNB), (0, CORE, CORE), (XNB, CORE, 3),
                                     (YNB, CORE, 5)):
            la[dst] = hop(la[src], mask)
            lb[dst] = hop(lb[src], mask)
        la[6] = hop(la[YNB], XNB)
        lb[6] = hop(lb[XNB], YNB)
        la[7] = hop(la[6], CORE)
        lb[7] = hop(lb[6], CORE)
        lora = jnp.stack([lb[d] for d in range(n_tp)])
        a_all = jnp.take(jnp.stack([la[d] for d in range(n_tp)]), jnp.bitwise_xor(me, jnp.arange(n_tp)), axis=0)
        a_qkv = jnp.transpose(a_all[:, :3], (2, 1, 0, 3)).reshape(n_ad, 3 * rank, dim)
        a_gu = jnp.transpose(a_all[:, 3:], (2, 1, 0, 3)).reshape(n_ad, 2 * rank, dim)
        mlp_pack = jnp.concatenate([b_gate, b_up, t_last(a_down)], axis=2)

        w_qkv = jnp.concatenate([w_q.reshape(dim, qw), w_k.reshape(dim, kw), w_v.reshape(dim, kw)], axis=1)
        att = {0: (w_qkv, w_o.reshape(qw, dim))}

        def move(pieces, src, mask):
            pieces[src ^ mask] = tuple(hop(v, mask) for v in pieces[src])

        move(att, 0, YNB)
        move(att, 0, XNB)
        move(att, 0, CORE)
        move(att, YNB, XNB)
        move(att, XNB, CORE)
        move(att, YNB, CORE)
        move(att, YNB ^ XNB, CORE)
        mlp = {0: (w_gate, w_up, w_down, mlp_pack)}
        move(mlp, 0, YNB)
        move(mlp, 0, CORE)
        move(mlp, YNB, CORE)
        mlp_order = (0, CORE, YNB, YNB ^ CORE)

        h, t_qkv = kernel_call(
            prep_body, (per,),
            [pl.BlockSpec((1, seq, dim), lambda i, m: (m[0] * per + i, 0, 0)),
             pl.BlockSpec((1, dim), lambda i, m: (0, 0)),
             pl.BlockSpec((1, 3 * rank, dim), lambda i, m: (m[own0 + i], 0, 0))],
            [pl.BlockSpec((1, seq, dim), lambda i, m: (i, 0, 0)),
             pl.BlockSpec((1, seq, 3 * rank), lambda i, m: (i, 0, 0))],
            [jax.ShapeDtypeStruct((per, seq, dim), BF16), jax.ShapeDtypeStruct((per, seq, 3 * rank), BF16)],
            [], 2 * per * seq * dim * 256, 4 * per * seq * dim,
        )(meta, x_in, gain_attn[None], a_qkv)

        def attn(ds, first, n):
            k = len(ds)
            return kernel_call(
                functools.partial(attn_body, scale, hd, rank, k), (n,),
                [pl.BlockSpec((1, seq, dim), lambda i, m: (first + i, 0, 0)),
                 pl.BlockSpec((1, seq, 3 * rank), lambda i, m: (first + i, 0, 0))]
                + [pl.BlockSpec((dim, cols), lambda i, m: (0, 0))] * k
                + [pl.BlockSpec((1, 1, rank, lora.shape[3]), lambda i, m, d=d: (d, m[own0 + first + i], 0, 0))
                   for d in ds],
                [pl.BlockSpec((1, seq, qw), lambda i, m: (i, 0, 0))] * k,
                [jax.ShapeDtypeStruct((n, seq, qw), BF16)] * k,
                [], 2 * k * n * seq * dim * cols * 2, 2 * k * (n * seq * (dim + qw) + dim * cols),
            )(meta, h, t_qkv, *[att[d][0] for d in ds], *[lora] * k)

        whole = {}
        for ds in ((0, 1), (2, 4), (3, 5)):
            whole.update(zip(ds, attn(ds, 0, per)))
        x1, x1n = [], []
        blk, ext = 512, 128
        for i in range(per):
            parts = [whole[d] for d in range(6)] + list(attn((6, 7), i, 1))
            x1.append(kernel_call(
                functools.partial(oproj_body, n_tp, scale, qw, cols, 2 * blk, ext), (1,),
                [pl.BlockSpec((1, seq, qw), lambda g, m, i=i if d < 6 else 0: (i, 0, 0)) for d in range(n_tp)]
                + [any_spec()] * n_tp
                + [pl.BlockSpec((1, seq, dim), lambda g, m, i=i: (m[0] * per + i, 0, 0)),
                   pl.BlockSpec((n_tp, 1, rank, lora.shape[3]), lambda g, m, i=i: (0, m[own0 + i], 0, 0))],
                pl.BlockSpec((seq, dim), lambda g, m: (0, 0)),
                jax.ShapeDtypeStruct((seq, dim), BF16),
                [pltpu.VMEM((seq, dim + ext), BF16), pltpu.VMEM((rank, dim), BF16), pltpu.VMEM((ext, dim), BF16),
                 pltpu.VMEM((2, dim + ext, 2 * blk), BF16), pltpu.SemaphoreType.DMA((2,))],
                2 * seq * dim * dim, 2 * (4 * seq * dim + dim * dim),
            )(meta, *parts, *[att[d][1] for d in range(n_tp)], x_in, lora))
            x1n.append(hop(x1[i], XNB))

        n_p = len(mlp_order)
        full = lambda g, m: (0, 0)

        def gate_up(j):
            return kernel_call(
                functools.partial(gu_body, n_p, scale, rank, blk, ext, j % 2), (1,),
                [any_spec(), any_spec(), pl.BlockSpec((1, dim), full),
                 pl.BlockSpec((1, 2 * rank, dim), lambda g, m: (m[slot0 + j], 0, 0))]
                + [pl.BlockSpec((1, rank, 3 * ff), lambda g, m: (m[slot0 + j], 0, 0))] * n_p
                + [any_spec()] * (2 * n_p),
                pl.BlockSpec((seq, n_p * ff), full),
                jax.ShapeDtypeStruct((seq, n_p * ff), BF16),
                [pltpu.VMEM((seq, dim + ext), BF16), pltpu.VMEM((2, ext, n_p * ff), BF16),
                 pltpu.VMEM((2, 2, dim + ext, blk), BF16), pltpu.VMEM((2, seq, blk), BF16),
                 pltpu.SemaphoreType.DMA((2, 2)), pltpu.SemaphoreType.DMA],
                4 * seq * dim * n_p * ff, 2 * (seq * (dim + n_p * ff) + 2 * dim * n_p * ff),
            )(meta, x1[j // 2], x1n[j // 2], gain_mlp[None], a_gu, *[mlp[d][3] for d in mlp_order],
              *[mlp[d][0] for d in mlp_order], *[mlp[d][1] for d in mlp_order])

        def down(mid, d):
            chunks = [CHUNKS[c] for c in DOWNS[d]]
            j, row0 = chunks[0][:2]
            splits = [c[2] for c in chunks]
            rows = sum(splits)
            outs = kernel_call(
                functools.partial(down_body, n_p, 2 * blk, 2 * ff, splits), (1,),
                [pl.BlockSpec((rows, n_p * ff), lambda g, m: (row0 // rows, 0))]
                + [pl.BlockSpec((1, rank, 3 * ff), lambda g, m: (m[slot0 + j], 0, 0))] * n_p + [any_spec()] * n_p,
                [pl.BlockSpec((n, dim), full) for n in splits] + [pl.BlockSpec((rank, n), full) for n in splits],
                [jax.ShapeDtypeStruct((n, dim), BF16) for n in splits]
                + [jax.ShapeDtypeStruct((rank, n), F32) for n in splits],
                [pltpu.VMEM((rank, n_p * ff), BF16), pltpu.VMEM((2, n_p * ff, 2 * blk), BF16),
                 pltpu.SemaphoreType.DMA((2,))],
                2 * rows * dim * n_p * ff, 2 * (rows * (dim + n_p * ff) + dim * n_p * ff),
            )(meta, mid, *[mlp[d][3] for d in mlp_order], *[mlp[d][2] for d in mlp_order])
            return list(zip(outs[:len(splits)], outs[len(splits):]))

        def final(c, pa, pb, ta, tb):
            j, row0, rows = CHUNKS[c]
            sub = 128
            at = lambda i, m: (i, 0)
            return kernel_call(
                functools.partial(fin_body, scale, cols + 2 * qw, qw, j % 2, row0), (rows // sub,),
                [pl.BlockSpec((sub, dim), at)] * 2 + [pl.BlockSpec((rank, sub), lambda i, m: (0, i))] * 2
                + [pl.BlockSpec((n_tp, 1, rank, lora.shape[3]), lambda g, m: (0, m[slot0 + j], 0, 0)),
                   any_spec(), any_spec()],
                pl.BlockSpec((sub, dim), at), jax.ShapeDtypeStruct((rows, dim), BF16),
                [pltpu.VMEM((rows, dim), BF16), pltpu.VMEM((rank, dim), BF16),
                 pltpu.SemaphoreType.DMA((rows // sub,))],
                2 * rows * dim * 256, 8 * rows * dim,
            )(meta, pa, pb, ta, tb, lora, x1[j // 2], x1n[j // 2])

        def place(buf, c, pieces):
            j, row0, rows = CHUNKS[c]
            masks = list(pieces)
            n = len(masks)

            def body(meta, *refs):
                src, dst, vbuf, sem_in, sem_out = refs[:n], refs[n + 1], refs[n + 2], refs[n + 3], refs[n + 4]
                base = meta[0] + (j % 2 - meta[1]) * XNB
                ins = [pltpu.make_async_copy(src[k], vbuf.at[k], sem_in.at[k]) for k in range(n)]
                outs = [pltpu.make_async_copy(
                    vbuf.at[k], dst.at[jnp.bitwise_xor(base, masks[k]) * per + j // 2, pl.ds(row0, rows)],
                    sem_out.at[k]) for k in range(n)]
                for cp in ins:
                    cp.start()
                for k in range(n):
                    ins[k].wait()
                    outs[k].start()
                for cp in outs:
                    cp.wait()

            return pl.pallas_call(
                body,
                grid_spec=pltpu.PrefetchScalarGridSpec(
                    num_scalar_prefetch=1, grid=(1,), in_specs=[any_spec()] * (n + 1), out_specs=any_spec(),
                    scratch_shapes=[pltpu.VMEM((n, rows, dim), BF16), pltpu.SemaphoreType.DMA((n,)),
                                    pltpu.SemaphoreType.DMA((n,))]),
                out_shape=jax.ShapeDtypeStruct(buf.shape, BF16),
                input_output_aliases={n + 1: 0},
                compiler_params=pltpu.CompilerParams(vmem_limit_bytes=VMEM_LIMIT),
                cost_estimate=pl.CostEstimate(flops=10 ** 9, bytes_accessed=4 * n * rows * dim, transcendentals=0))(meta, *[pieces[d] for d in masks], buf)

        out = pl.pallas_call(lambda o_ref: None, out_shape=jax.ShapeDtypeStruct(x_in.shape, BF16),
                             out_specs=any_spec(), name="buffer")()
        mids = [gate_up(j) for j in range(2 * per)]
        for d, chunk_ids in enumerate(DOWNS):
            for c, (pa, ta) in zip(chunk_ids, down(mids[CHUNKS[chunk_ids[0]][0]], d)):
                tb, pb = hop(ta, XNB), hop(pa, XNB)
                y = final(c, pa, pb, ta, tb)
                yy = hop(y, YNB)
                out = place(out, c, {0: y, CORE: hop(y, CORE), YNB: yy, YNB ^ CORE: hop(yy, CORE)})
        return out

    return jax.shard_map(local_layer, mesh=mesh, in_specs=in_specs, out_specs=act_spec, check_vma=False)
```

```python
import functools

import jax
import jax.numpy as jnp
from jax import lax
from jax.experimental import pallas as pl
from jax.experimental.pallas import tpu as pltpu
from jax.sharding import PartitionSpec as P


LORA_ALPHA = 16
RMS_EPS = 1e-5
F32 = jnp.float32
BF16 = jnp.bfloat16
CORE, XNB, YNB = 1, 2, 4
VMEM_LIMIT = 60 * 1024 * 1024

CHUNKS = ([(0, 0, 128), (0, 128, 128), (0, 256, 256)] + [(j, 0, 512) for j in range(1, 7)]
          + [(7, 0, 256), (7, 256, 128), (7, 384, 128)])
DOWNS = [(0, 1), (2,), (3,), (4,), (5,), (6,), (7,), (8,), (9, 10, 11)]


def dot_nt(a, b):
    return lax.dot_general(a, b, (((1,), (1,)), ((), ())), preferred_element_type=F32)


def dot_nn(a, b):
    return lax.dot_general(a, b, (((1,), (0,)), ((), ())), preferred_element_type=F32)


def kernel_call(body, grid, in_specs, out_specs, out_shape, scratch, flops, nbytes):
    return pl.pallas_call(
        body,
        grid_spec=pltpu.PrefetchScalarGridSpec(num_scalar_prefetch=1, grid=grid, in_specs=in_specs,
                                               out_specs=out_specs, scratch_shapes=scratch),
        out_shape=out_shape,
        compiler_params=pltpu.CompilerParams(vmem_limit_bytes=VMEM_LIMIT),
        cost_estimate=pl.CostEstimate(flops=int(flops), bytes_accessed=int(nbytes), transcendentals=0))


def any_spec():
    return pl.BlockSpec(memory_space=pl.ANY)


def prep_body(meta, x_ref, g_ref, a_ref, h_ref, t_ref):
    xv = x_ref[0].astype(F32)
    inv = lax.rsqrt(jnp.mean(xv * xv, axis=-1, keepdims=True) + RMS_EPS)
    hv = (xv * inv * g_ref[...]).astype(BF16)
    h_ref[0] = hv
    t_ref[0] = dot_nt(hv, a_ref[0]).astype(BF16)


def rank_dot(a, b):
    n = a.shape[0] // 2
    return jnp.concatenate([dot_nt(a[:n], b), dot_nt(a[n:], b)], axis=0)


def softmax_bf16(blocks, scale):
    m = functools.reduce(jnp.maximum, [jnp.max(s, axis=-1, keepdims=True) for s in blocks])
    e = [jnp.exp2((s - m) * (scale * 1.4426950408889634)) for s in blocks]
    inv = 1.0 / functools.reduce(jnp.add, [jnp.sum(v, axis=-1, keepdims=True) for v in e])
    return [(v * inv).astype(BF16) for v in e]


def attn_body(scale, hd, rank, n_w, meta, h_ref, t_ref, *refs):
    w_refs, l_refs, o_refs = refs[:n_w], refs[n_w:2 * n_w], refs[2 * n_w:]
    seq = h_ref.shape[1]
    cols = w_refs[0].shape[1]
    qw = cols - 2 * hd
    half = seq // 2
    row = lax.broadcasted_iota(jnp.int32, (3 * rank, cols), 0) // rank
    col = lax.broadcasted_iota(jnp.int32, (3 * rank, cols), 1)
    part = jnp.where(col < qw, 0, jnp.where(col < qw + hd, 1, 2))
    keep = (lax.broadcasted_iota(jnp.int32, (half, half), 0) >= lax.broadcasted_iota(jnp.int32, (half, half), 1))
    zs = []
    for w_ref, l_ref in zip(w_refs, l_refs):
        bl = l_ref[0, 0][:, :cols]
        bd = jnp.where(row == part, jnp.concatenate([bl, bl, bl], axis=0), jnp.zeros((), BF16))
        zs.append((dot_nn(h_ref[0], w_ref[...]) + scale * dot_nn(t_ref[0], bd)).astype(BF16))
    for z, o_ref in zip(zs, o_refs):
        k = [z[r * half:(r + 1) * half, qw:qw + hd] for r in range(2)]
        v = [z[r * half:(r + 1) * half, qw + hd:] for r in range(2)]
        for j in range(qw // hd):
            for r in range(2):
                q = z[r * half:(r + 1) * half, j * hd:(j + 1) * hd]
                s = [dot_nt(q, k[c]) for c in range(r + 1)]
                s[r] = jnp.where(keep, s[r], -jnp.inf)
                p = softmax_bf16(s, hd ** -0.5)
                o = functools.reduce(jnp.add, [dot_nn(p[c], v[c]) for c in range(r + 1)])
                o_ref[0, r * half:(r + 1) * half, j * hd:(j + 1) * hd] = o.astype(BF16)


def twice(scale, t):
    return [t] * int(scale)


def oproj_body(n_tp, scale, qw, cols0, blk, ext, meta, *refs):
    o_refs, w_refs = refs[:n_tp], refs[n_tp:2 * n_tp]
    x_ref, l_ref, x1_ref, ocat, acat, bcat, wbuf, sems = refs[2 * n_tp:]
    dim = x1_ref.shape[1]
    rank = acat.shape[0]
    n_blk = dim // blk
    me = meta[0]

    def copies(n, slot):
        return [pltpu.make_async_copy(w_refs[p].at[:, pl.ds(n * blk, blk)], wbuf.at[slot, pl.ds(p * qw, qw)],
                                      sems.at[slot]) for p in range(n_tp)]

    for c in copies(0, 0):
        c.start()
    bcat[...] = jnp.zeros_like(bcat)
    for p in range(n_tp):
        ocat[:, p * qw:(p + 1) * qw] = o_refs[p][0]
        acat[:, p * qw:(p + 1) * qw] = l_ref[p, 0, :, cols0:cols0 + qw]
        b = l_ref[jnp.bitwise_xor(me, p), 0, :, cols0 + qw:cols0 + 2 * qw]
        bcat[:2 * rank, p * qw:(p + 1) * qw] = jnp.concatenate(twice(scale, b), axis=0)
    t = rank_dot(ocat[:, :dim], acat[...]).astype(BF16)
    pad = jnp.zeros((t.shape[0], ext - 2 * rank), BF16)
    ocat[:, dim:] = jnp.concatenate(twice(scale, t) + [pad], axis=1)

    @pl.loop(0, n_blk)
    def _(n):
        slot = lax.rem(n, 2)

        @pl.when(n + 1 < n_blk)
        def _():
            for c in copies(n + 1, 1 - slot):
                c.start()

        cols = pl.ds(pl.multiple_of(n * blk, blk), blk)
        wbuf[slot, dim:] = bcat[:, cols]
        for c in copies(n, slot):
            c.wait()
        z = dot_nn(ocat[...], wbuf[slot])
        x1_ref[:, cols] = (x_ref[0, :, cols].astype(F32) + z).astype(BF16)


def row_copies(src, dst, sem, parts):
    n = src.shape[0] // parts
    return [pltpu.make_async_copy(src.at[pl.ds(k * n, n)], dst.at[pl.ds(k * n, n)], sem) for k in range(parts)]


def pick(meta, which, own_ref, nbr_ref, dst, sem, parts):
    own = meta[1] == which

    @pl.when(own)
    def _():
        for c in row_copies(own_ref, dst, sem, parts):
            c.start()

    @pl.when(jnp.logical_not(own))
    def _():
        for c in row_copies(nbr_ref, dst, sem, parts):
            c.start()


def gu_body(n_p, scale, rank, blk, ext, which, meta, xo_ref, xn_ref, g_ref, a_ref, *refs):
    b_refs, g_refs, u_refs = refs[:n_p], refs[n_p:2 * n_p], refs[2 * n_p:3 * n_p]
    m_ref, hbuf, bcat, wbuf, zbuf, sems, sem_x = refs[3 * n_p:]
    ff = g_refs[0].shape[1]
    dim = xo_ref.shape[1]
    per = ff // blk
    n_blk = n_p * per

    def start(j, slot):
        for p in range(n_p):
            @pl.when(j // per == p)
            def _():
                cols = pl.ds(pl.multiple_of(lax.rem(j, per) * blk, blk), blk)
                for i, w in enumerate((g_refs[p], u_refs[p])):
                    for c in row_copies(w.at[:, cols], wbuf.at[slot, i, pl.ds(0, dim)], sems.at[slot, i], 4):
                        c.start()

    pick(meta, which, xo_ref, xn_ref, hbuf.at[:, pl.ds(0, dim)], sem_x, 4)
    start(0, 0)
    zero = jnp.zeros((2 * rank, ff), BF16)
    rest = jnp.zeros((ext - 4 * rank, ff), BF16)
    for p in range(n_p):
        bg = twice(scale, b_refs[p][0, :, :ff])
        bu = twice(scale, b_refs[p][0, :, ff:2 * ff])
        bcat[0, :, p * ff:(p + 1) * ff] = jnp.concatenate(bg + [zero, rest], axis=0)
        bcat[1, :, p * ff:(p + 1) * ff] = jnp.concatenate([zero] + bu + [rest], axis=0)
    pltpu.make_async_copy(xo_ref, hbuf.at[:, pl.ds(0, dim)], sem_x).wait()
    xv = hbuf[:, :dim].astype(F32)
    inv = lax.rsqrt(jnp.mean(xv * xv, axis=-1, keepdims=True) + RMS_EPS)
    hbuf[:, :dim] = (xv * inv * g_ref[...]).astype(BF16)
    t = rank_dot(hbuf[:, :dim], a_ref[0]).astype(BF16)
    pad = jnp.zeros((t.shape[0], ext - 4 * rank), BF16)
    hbuf[:, dim:] = jnp.concatenate(twice(scale, t[:, :rank]) + twice(scale, t[:, rank:]) + [pad], axis=1)

    def act(j):
        gate, up = zbuf[0].astype(F32), zbuf[1].astype(F32)
        m_ref[:, pl.ds(pl.multiple_of(j * blk, blk), blk)] = (jax.nn.silu(gate) * up).astype(BF16)

    zbuf[...] = jnp.zeros_like(zbuf)

    @pl.loop(0, n_blk)
    def _(j):
        slot = lax.rem(j, 2)

        @pl.when(j + 1 < n_blk)
        def _():
            start(j + 1, 1 - slot)

        cols = pl.ds(pl.multiple_of(j * blk, blk), blk)
        for i in range(2):
            wbuf[slot, i, dim:] = bcat[i, :, cols]
            pltpu.make_async_copy(g_refs[0].at[:, pl.ds(0, blk)], wbuf.at[slot, i, pl.ds(0, dim)],
                                  sems.at[slot, i]).wait()
        act(jnp.maximum(j - 1, 0))
        for i in range(2):
            zbuf[i] = dot_nn(hbuf[...], wbuf[slot, i]).astype(BF16)

    act(n_blk - 1)


def down_body(n_p, blk, b_off, splits, meta, m_ref, *refs):
    b_refs, d_refs = refs[:n_p], refs[n_p:2 * n_p]
    refs = refs[2 * n_p:]
    k = len(splits)
    p_refs, t_refs, (acat, wbuf, sems) = refs[:k], refs[k:2 * k], refs[2 * k:]
    ff, dim = d_refs[0].shape
    n_blk = dim // blk

    def copies(n, slot):
        return [c for p in range(n_p) for c in row_copies(d_refs[p].at[:, pl.ds(n * blk, blk)],
                                                          wbuf.at[slot, pl.ds(p * ff, ff)], sems.at[slot], 2)]

    for c in copies(0, 0):
        c.start()
    for p in range(n_p):
        acat[:, p * ff:(p + 1) * ff] = b_refs[p][0, :, b_off:b_off + ff]
    t = rank_dot(m_ref[...], acat[...]).T
    row = 0
    for n, t_ref in zip(splits, t_refs):
        t_ref[...] = t[:, row:row + n]
        row += n

    @pl.loop(0, n_blk)
    def _(n):
        slot = lax.rem(n, 2)

        @pl.when(n + 1 < n_blk)
        def _():
            for c in copies(n + 1, 1 - slot):
                c.start()

        for c in copies(n, slot):
            c.wait()
        z = dot_nn(m_ref[...], wbuf[slot]).astype(BF16)
        row = 0
        for rows, p_ref in zip(splits, p_refs):
            p_ref[:, pl.ds(pl.multiple_of(n * blk, blk), blk)] = z[row:row + rows]
            row += rows


def fin_body(scale, l_off, qw, which, row0, sub, meta, pa_ref, pb_ref, ta_ref, tb_ref, l_ref, xo_ref, xn_ref,
             y_ref, buf, ybuf, bcat, sem_in, sem_out):
    n_rows = ybuf.shape[0]
    n = n_rows // sub
    for b in range(n):
        dst = pl.ds(b * sub, sub)
        pltpu.make_async_copy(pa_ref.at[dst], buf.at[0, dst], sem_in.at[b]).start()
        pltpu.make_async_copy(pb_ref.at[dst], buf.at[1, dst], sem_in.at[b]).start()
        src = pl.ds(row0 + b * sub, sub)
        pick(meta, which, xo_ref.at[src], xn_ref.at[src], buf.at[2, dst], sem_in.at[b], 1)
    for p in range(l_ref.shape[0]):
        bcat[:, p * qw:(p + 1) * qw] = l_ref[jnp.bitwise_xor(meta[0], p), 0, :, l_off:l_off + qw]
    t = (ta_ref[...] + tb_ref[...]).T.astype(BF16)
    outs = []
    for b in range(n):
        dst = pl.ds(b * sub, sub)
        for k in range(3):
            pltpu.make_async_copy(pa_ref.at[dst], buf.at[k, dst], sem_in.at[b]).wait()
        rows = slice(b * sub, (b + 1) * sub)
        z = buf[0, rows].astype(F32) + buf[1, rows].astype(F32) + scale * dot_nn(t[rows], bcat[...])
        ybuf[rows] = (buf[2, rows].astype(F32) + z).astype(BF16)
        outs.append(pltpu.make_async_copy(ybuf.at[dst], y_ref.at[dst], sem_out.at[b]))
        outs[-1].start()
    for c in outs:
        c.wait()


def solution(mesh):
    act_spec = P('dp', None, None)
    w_head_spec = P(None, 'tp', None)
    w_out_spec = P('tp', None, None)
    w_col_spec = P(None, 'tp')
    w_row_spec = P('tp', None)
    a_rank_spec = P(None, None, 'tp')
    b_head_spec = P(None, None, 'tp', None)
    b_col_spec = P(None, None, 'tp')
    a_head_spec = P(None, 'tp', None, None)
    a_row_spec = P(None, 'tp', None)
    in_specs = (act_spec, P('dp'), P(None), P(None), w_head_spec, w_head_spec, w_head_spec, w_out_spec,
                w_col_spec, w_col_spec, w_row_spec, a_rank_spec, b_head_spec, a_rank_spec, b_head_spec,
                a_rank_spec, b_head_spec, a_head_spec, b_col_spec, a_rank_spec, b_col_spec,
                a_rank_spec, b_col_spec, a_row_spec, b_col_spec)
    n_tp = mesh.shape['tp']

    def local_layer(x_in, adapter_ids, gain_attn, gain_mlp, w_q, w_k, w_v, w_o, w_gate, w_up, w_down,
                    a_q, b_q, a_k, b_k, a_v, b_v, a_o, b_o, a_gate, b_gate, a_up, b_up, a_down, b_down):
        num_seqs, seq, dim = x_in.shape
        hd = w_q.shape[2]
        n_ad, rank = b_q.shape[:2]
        scale = LORA_ALPHA / rank
        per = num_seqs // n_tp
        ff = w_gate.shape[1]
        qw, kw = w_q.shape[1] * hd, w_k.shape[1] * hd
        cols = qw + 2 * kw
        me = lax.axis_index('tp')

        def hop(v, mask):
            return lax.ppermute(v, 'tp', [(i, i ^ mask) for i in range(n_tp)])

        def t_last(a):
            return jnp.swapaxes(a, -1, -2)

        ids_own = lax.dynamic_slice_in_dim(adapter_ids, me * per, per)
        xbit = (me // XNB) % 2
        ids_w = [lax.dynamic_slice_in_dim(adapter_ids, (me + (w - xbit) * XNB) * per, per) for w in range(2)]
        meta = jnp.concatenate([jnp.stack([me, xbit]).astype(jnp.int32), ids_own, jnp.stack(ids_w, axis=1).reshape(-1)])
        own0, slot0 = 2, 2 + per

        lora_pack = jnp.concatenate([
            b_q.reshape(n_ad, rank, qw), b_k.reshape(n_ad, rank, kw), b_v.reshape(n_ad, rank, kw),
            t_last(a_o.reshape(n_ad, qw, rank)), b_o, b_down], axis=2)
        a_pack = jnp.stack([a_q[:, :, 0], a_k[:, :, 0], a_v[:, :, 0], a_gate[:, :, 0], a_up[:, :, 0]], axis=0)
        la, lb = {0: a_pack}, {0: lora_pack}
        for src, mask, dst in ((0, YNB, YNB), (0, XNB, XNB), (0, CORE, CORE), (XNB, CORE, 3),
                                     (YNB, CORE, 5)):
            la[dst] = hop(la[src], mask)
            lb[dst] = hop(lb[src], mask)
        la[6] = hop(la[YNB], XNB)
        lb[6] = hop(lb[XNB], YNB)
        la[7] = hop(la[6], CORE)
        lb[7] = hop(lb[6], CORE)
        lora = jnp.stack([lb[d] for d in range(n_tp)])
        a_all = jnp.take(jnp.stack([la[d] for d in range(n_tp)]), jnp.bitwise_xor(me, jnp.arange(n_tp)), axis=0)
        a_qkv = jnp.transpose(a_all[:, :3], (2, 1, 0, 3)).reshape(n_ad, 3 * rank, dim)
        a_gu = jnp.transpose(a_all[:, 3:], (2, 1, 0, 3)).reshape(n_ad, 2 * rank, dim)
        mlp_pack = jnp.concatenate([b_gate, b_up, t_last(a_down)], axis=2)

        w_qkv = jnp.concatenate([w_q.reshape(dim, qw), w_k.reshape(dim, kw), w_v.reshape(dim, kw)], axis=1)
        att = {0: (w_qkv, w_o.reshape(qw, dim))}

        def move(pieces, src, mask):
            pieces[src ^ mask] = tuple(hop(v, mask) for v in pieces[src])

        move(att, 0, YNB)
        move(att, 0, XNB)
        move(att, 0, CORE)
        move(att, YNB, XNB)
        move(att, XNB, CORE)
        move(att, YNB, CORE)
        move(att, YNB ^ XNB, CORE)
        mlp = {0: (w_gate, w_up, w_down, mlp_pack)}
        move(mlp, 0, YNB)
        move(mlp, 0, CORE)
        move(mlp, YNB, CORE)
        mlp_order = (0, CORE, YNB, YNB ^ CORE)

        h, t_qkv = kernel_call(
            prep_body, (per,),
            [pl.BlockSpec((1, seq, dim), lambda i, m: (m[0] * per + i, 0, 0)),
             pl.BlockSpec((1, dim), lambda i, m: (0, 0)),
             pl.BlockSpec((1, 3 * rank, dim), lambda i, m: (m[own0 + i], 0, 0))],
            [pl.BlockSpec((1, seq, dim), lambda i, m: (i, 0, 0)),
             pl.BlockSpec((1, seq, 3 * rank), lambda i, m: (i, 0, 0))],
            [jax.ShapeDtypeStruct((per, seq, dim), BF16), jax.ShapeDtypeStruct((per, seq, 3 * rank), BF16)],
            [], 2 * per * seq * dim * 256, 4 * per * seq * dim,
        )(meta, x_in, gain_attn[None], a_qkv)

        def attn(ds, first, n):
            k = len(ds)
            return kernel_call(
                functools.partial(attn_body, scale, hd, rank, k), (n,),
                [pl.BlockSpec((1, seq, dim), lambda i, m: (first + i, 0, 0)),
                 pl.BlockSpec((1, seq, 3 * rank), lambda i, m: (first + i, 0, 0))]
                + [pl.BlockSpec((dim, cols), lambda i, m: (0, 0))] * k
                + [pl.BlockSpec((1, 1, rank, lora.shape[3]), lambda i, m, d=d: (d, m[own0 + first + i], 0, 0))
                   for d in ds],
                [pl.BlockSpec((1, seq, qw), lambda i, m: (i, 0, 0))] * k,
                [jax.ShapeDtypeStruct((n, seq, qw), BF16)] * k,
                [], 2 * k * n * seq * dim * cols * 2, 2 * k * (n * seq * (dim + qw) + dim * cols),
            )(meta, h, t_qkv, *[att[d][0] for d in ds], *[lora] * k)

        whole = {}
        for ds in ((0, 1), (2, 4), (3, 5)):
            whole.update(zip(ds, attn(ds, 0, per)))
        x1, x1n = [], []
        blk, ext = 512, 128
        for i in range(per):
            parts = [whole[d] for d in range(6)] + list(attn((6, 7), i, 1))
            x1.append(kernel_call(
                functools.partial(oproj_body, n_tp, scale, qw, cols, blk, ext), (1,),
                [pl.BlockSpec((1, seq, qw), lambda g, m, i=i if d < 6 else 0: (i, 0, 0)) for d in range(n_tp)]
                + [any_spec()] * n_tp
                + [pl.BlockSpec((1, seq, dim), lambda g, m, i=i: (m[0] * per + i, 0, 0)),
                   pl.BlockSpec((n_tp, 1, rank, lora.shape[3]), lambda g, m, i=i: (0, m[own0 + i], 0, 0))],
                pl.BlockSpec((seq, dim), lambda g, m: (0, 0)),
                jax.ShapeDtypeStruct((seq, dim), BF16),
                [pltpu.VMEM((seq, dim + ext), BF16), pltpu.VMEM((rank, dim), BF16), pltpu.VMEM((ext, dim), BF16),
                 pltpu.VMEM((2, dim + ext, blk), BF16), pltpu.SemaphoreType.DMA((2,))],
                2 * seq * dim * dim, 2 * (4 * seq * dim + dim * dim),
            )(meta, *parts, *[att[d][1] for d in range(n_tp)], x_in, lora))
            x1n.append(hop(x1[i], XNB))

        n_p = len(mlp_order)
        full = lambda g, m: (0, 0)

        def gate_up(j):
            return kernel_call(
                functools.partial(gu_body, n_p, scale, rank, blk, ext, j % 2), (1,),
                [any_spec(), any_spec(), pl.BlockSpec((1, dim), full),
                 pl.BlockSpec((1, 2 * rank, dim), lambda g, m: (m[slot0 + j], 0, 0))]
                + [pl.BlockSpec((1, rank, 3 * ff), lambda g, m: (m[slot0 + j], 0, 0))] * n_p
                + [any_spec()] * (2 * n_p),
                pl.BlockSpec((seq, n_p * ff), full),
                jax.ShapeDtypeStruct((seq, n_p * ff), BF16),
                [pltpu.VMEM((seq, dim + ext), BF16), pltpu.VMEM((2, ext, n_p * ff), BF16),
                 pltpu.VMEM((2, 2, dim + ext, blk), BF16), pltpu.VMEM((2, seq, blk), BF16),
                 pltpu.SemaphoreType.DMA((2, 2)), pltpu.SemaphoreType.DMA],
                4 * seq * dim * n_p * ff, 2 * (seq * (dim + n_p * ff) + 2 * dim * n_p * ff),
            )(meta, x1[j // 2], x1n[j // 2], gain_mlp[None], a_gu, *[mlp[d][3] for d in mlp_order],
              *[mlp[d][0] for d in mlp_order], *[mlp[d][1] for d in mlp_order])

        def down(mid, d):
            chunks = [CHUNKS[c] for c in DOWNS[d]]
            j, row0 = chunks[0][:2]
            splits = [c[2] for c in chunks]
            rows = sum(splits)
            outs = kernel_call(
                functools.partial(down_body, n_p, blk, 2 * ff, splits), (1,),
                [pl.BlockSpec((rows, n_p * ff), lambda g, m: (row0 // rows, 0))]
                + [pl.BlockSpec((1, rank, 3 * ff), lambda g, m: (m[slot0 + j], 0, 0))] * n_p + [any_spec()] * n_p,
                [pl.BlockSpec((n, dim), full) for n in splits] + [pl.BlockSpec((rank, n), full) for n in splits],
                [jax.ShapeDtypeStruct((n, dim), BF16) for n in splits]
                + [jax.ShapeDtypeStruct((rank, n), F32) for n in splits],
                [pltpu.VMEM((rank, n_p * ff), BF16), pltpu.VMEM((2, n_p * ff, blk), BF16),
                 pltpu.SemaphoreType.DMA((2,))],
                2 * rows * dim * n_p * ff, 2 * (rows * (dim + n_p * ff) + dim * n_p * ff),
            )(meta, mid, *[mlp[d][3] for d in mlp_order], *[mlp[d][2] for d in mlp_order])
            return list(zip(outs[:len(splits)], outs[len(splits):]))

        def final(c, pa, pb, ta, tb):
            j, row0, rows = CHUNKS[c]
            sub = 128
            return kernel_call(
                functools.partial(fin_body, scale, cols + 2 * qw, qw, j % 2, row0, sub), (1,),
                [any_spec()] * 2 + [pl.BlockSpec((rank, rows), full)] * 2
                + [pl.BlockSpec((n_tp, 1, rank, lora.shape[3]), lambda g, m: (0, m[slot0 + j], 0, 0)),
                   any_spec(), any_spec()],
                any_spec(), jax.ShapeDtypeStruct((rows, dim), BF16),
                [pltpu.VMEM((3, rows, dim), BF16), pltpu.VMEM((rows, dim), BF16), pltpu.VMEM((rank, dim), BF16),
                 pltpu.SemaphoreType.DMA((rows // sub,)), pltpu.SemaphoreType.DMA((rows // sub,))],
                2 * rows * dim * 256, 8 * rows * dim,
            )(meta, pa, pb, ta, tb, lora, x1[j // 2], x1n[j // 2])

        def place(buf, c, pieces):
            j, row0, rows = CHUNKS[c]
            masks = list(pieces)
            n = len(masks)

            def body(meta, *refs):
                src, dst, vbuf, sem_in, sem_out = refs[:n], refs[n + 1], refs[n + 2], refs[n + 3], refs[n + 4]
                base = meta[0] + (j % 2 - meta[1]) * XNB
                ins = [pltpu.make_async_copy(src[k], vbuf.at[k], sem_in.at[k]) for k in range(n)]
                outs = [pltpu.make_async_copy(
                    vbuf.at[k], dst.at[jnp.bitwise_xor(base, masks[k]) * per + j // 2, pl.ds(row0, rows)],
                    sem_out.at[k]) for k in range(n)]
                for cp in ins:
                    cp.start()
                for k in range(n):
                    ins[k].wait()
                    outs[k].start()
                for cp in outs:
                    cp.wait()

            return pl.pallas_call(
                body,
                grid_spec=pltpu.PrefetchScalarGridSpec(
                    num_scalar_prefetch=1, grid=(1,), in_specs=[any_spec()] * (n + 1), out_specs=any_spec(),
                    scratch_shapes=[pltpu.VMEM((n, rows, dim), BF16), pltpu.SemaphoreType.DMA((n,)),
                                    pltpu.SemaphoreType.DMA((n,))]),
                out_shape=jax.ShapeDtypeStruct(buf.shape, BF16),
                input_output_aliases={n + 1: 0},
                compiler_params=pltpu.CompilerParams(vmem_limit_bytes=VMEM_LIMIT),
                cost_estimate=pl.CostEstimate(flops=10 ** 9, bytes_accessed=4 * n * rows * dim, transcendentals=0))(meta, *[pieces[d] for d in masks], buf)

        out = pl.pallas_call(lambda o_ref: None, out_shape=jax.ShapeDtypeStruct(x_in.shape, BF16),
                             out_specs=any_spec(), name="buffer")()
        mids = [gate_up(j) for j in range(2 * per)]
        for d, chunk_ids in enumerate(DOWNS):
            for c, (pa, ta) in zip(chunk_ids, down(mids[CHUNKS[chunk_ids[0]][0]], d)):
                tb, pb = hop(ta, XNB), hop(pa, XNB)
                y = final(c, pa, pb, ta, tb)
                yy = hop(y, YNB)
                out = place(out, c, {0: y, CORE: hop(y, CORE), YNB: yy, YNB ^ CORE: hop(yy, CORE)})
        return out

    return jax.shard_map(local_layer, mesh=mesh, in_specs=in_specs, out_specs=act_spec, check_vma=False)
```
